32 devices in a mesh: rep: 4 (over y, x), fsdp: 8 (over z, core).
Axes of the slice: x: 2, y: 2, z: 4, core: 2. Of those that a mesh axis runs over, the one named last changes fastest.
Arguments:
- tokens: bfloat16 [4096, 4096], P(('rep', 'fsdp')), may hold values from -6 to 6
- grad_out: bfloat16 [4096, 4096], P(('rep', 'fsdp')), may hold values from -6 to 6
- gate_weight: bfloat16 [4096, 512], P('fsdp'), may hold values from -0.09375 to 0.09375
- down_weight: bfloat16 [4096, 512], P('fsdp'), may hold values from -0.25 to 0.25
- residual_in: float32 [4, 4096, 512], P('rep', 'fsdp'), may hold values from -6 to 6
Outputs:
- residual_out: float32 [4, 4096, 512], P('rep', 'fsdp')
- update: float32 [4096, 512], P('fsdp')
The draws below stay inside these ranges and needn't reach their ends.
All inputs are finite; a program needn't handle non-finite values.
Results may differ from the reference program's by a relative error of at most 0.018.
Values may be sent and summed in bfloat16 or wider, within the bound.
No kernel may reach another device: no remote copies, remote signals or barrier semaphores. Data moves between devices by JAX's collectives and lax.ppermute only.
A program may use at most 64 MiB of HBM per device.

```python
import math
import jax
import jax.numpy as jnp
from jax import lax

D = 4096
FF = 512
TOK_DEV = 128
TOKENS = 4096
N_REP = 4
N_FSDP = 8


def steps_of(stream_key, extent, cuts, low, largest):
    gain, own = 1.0, jax.random.fold_in(stream_key, 6)
    for dim, blocks in cuts:
        heights = jnp.exp(jax.random.uniform(jax.random.fold_in(own, dim), (blocks,), jnp.float32, low / len(cuts), largest / len(cuts)))
        gain = gain * jnp.repeat(heights, extent[dim] // blocks).reshape([-1 if axis == dim else 1 for axis in range(len(extent))])
    return gain


def normal_values(own_key, dims, scale, most, shards=(), dtype=jnp.bfloat16):
    gain = steps_of(own_key, dims, shards, -0.22, 0.18) if shards else 1.0
    drawn = jax.random.normal(own_key, dims, jnp.float32) * scale * gain
    return jnp.minimum(jnp.maximum(drawn, -most), most).astype(dtype)


def setup_inputs(seed: int = 0) -> dict:
    key_of = jax.random.split(jax.random.key(seed), 6)
    tokens = normal_values(key_of[0], (TOKENS, D), 1.0, 6.0, ((0, 32),))
    grad_out = normal_values(key_of[1], (TOKENS, D), 1.0, 6.0, ((0, 32),))
    gate_weight = normal_values(key_of[2], (D, FF), D ** -0.5, 0.09375, ((0, 8),))
    down_weight = normal_values(key_of[3], (D, FF), FF ** -0.5, 0.25, ((0, 8),))
    residual_in = normal_values(key_of[4], (N_REP, D, FF), 1.0, 6.0, ((0, 4), (1, 8)), jnp.float32)
    return {"tokens": tokens, "grad_out": grad_out, "gate_weight": gate_weight, "down_weight": down_weight, "residual_in": residual_in}


def reference(tokens, grad_out, gate_weight, down_weight, residual_in):
    grouped = tokens.reshape(N_REP, N_FSDP, TOK_DEV, D)
    grouped_grad = grad_out.reshape(N_REP, N_FSDP, TOK_DEV, D)
    norm_factor = math.sqrt(TOK_DEV * N_FSDP)

    def one_block(carry, inputs):
        block_tokens, block_grad = inputs
        gate_pre = jnp.dot(block_tokens, gate_weight, preferred_element_type=jnp.float32)
        hidden_grad = jnp.dot(block_grad, down_weight, preferred_element_type=jnp.float32)
        up_grad = (hidden_grad * (gate_pre * jax.nn.sigmoid(gate_pre))).astype(jnp.bfloat16)
        term = jnp.dot(block_tokens.T, up_grad, preferred_element_type=jnp.float32)
        partial_term = lax.optimization_barrier(term.astype(jnp.bfloat16))
        return (carry + partial_term.astype(jnp.float32), None)

    def one_group(inputs):
        group_tokens, group_grad, group_residual = inputs
        start = jnp.zeros((D, FF), jnp.float32)
        summed, _ = lax.scan(one_block, start, (group_tokens, group_grad))
        total = summed / norm_factor + group_residual
        scale = (lax.optimization_barrier(jnp.mean(jnp.abs(total), axis=1)) + 1e-06).astype(jnp.bfloat16)
        scale_full = scale.astype(jnp.float32)[:, None]
        soft_sign = jnp.tanh(total / scale_full).astype(jnp.bfloat16)
        decoded = scale_full * soft_sign.astype(jnp.float32)
        return (total - decoded, decoded)
    residual_out, decoded_all = lax.map(one_group, (grouped, grouped_grad, residual_in))
    update = lax.optimization_barrier(jnp.sum(decoded_all, axis=0)) / N_REP
    return (residual_out, update)
```

```python
import math

import jax
import jax.numpy as jnp
from jax import lax
from jax.experimental import pallas as pl
from jax.experimental.pallas import tpu as pltpu
from jax.sharding import PartitionSpec as P

F32 = jnp.float32
BF16 = jnp.bfloat16


def gather_rep(piece, groups, swap):
    if groups == 4:
        from_x, from_y = swap(piece, 1), swap(piece, 2)
        return {
            0: {0: piece[0], 1: piece[1]},
            1: {0: from_x[0], 1: from_x[1]},
            2: {0: from_y[0], 1: from_y[1]},
            3: {0: swap(from_x[0], 2), 1: swap(from_y[1], 1)},
        }
    found = {0: {0: piece[0], 1: piece[1]}}
    bit = 1
    while bit < groups:
        for offset in list(found):
            found[offset ^ bit] = {w: swap(found[offset][w], bit) for w in (0, 1)}
        bit *= 2
    return found


def hidden_kernel(places, rows, pos_ref, t0, t1, g0, g1, *refs):
    weights, out = refs[:-1], refs[-1]
    sides = ((t0, t1), (g0, g1))
    acc = [None, None]
    for index, (ref, w) in enumerate(zip(weights, places)):
        start = pl.multiple_of(pos_ref[index], 128)
        first, second = sides[w]
        count = ref.shape[0]
        lhs = jnp.concatenate([first[:, pl.ds(start, count)], second[:, pl.ds(start, count)]], axis=0)
        term = jnp.dot(lhs, ref[...], preferred_element_type=F32)
        acc[w] = term if acc[w] is None else acc[w] + term
    gate, hidden = acc
    out[...] = (hidden * (gate * jax.nn.sigmoid(gate))).astype(BF16)


def update_kernel(norm, chips, core_ref, res, *refs):
    toks, mine, theirs = refs[:chips], refs[chips:2 * chips], refs[2 * chips:3 * chips]
    res_out, dec = refs[3 * chips:]
    rows, width = dec.shape
    half = width // 2
    dims = (((0,), (0,)), ((), ()))
    near = far = None
    for t, u, v in zip(toks, mine, theirs):
        block = t.shape[1]
        a, b = t[0], t[1]
        n = lax.dot_general(a, u[:block], dims, preferred_element_type=F32) + lax.dot_general(
            b, u[block:], dims, preferred_element_type=F32)
        m = lax.dot_general(a, v[block:], dims, preferred_element_type=F32) + lax.dot_general(
            b, v[:block], dims, preferred_element_type=F32)
        near = n if near is None else near + n
        far = m if far is None else far + m
    core = core_ref[0]
    here = pl.multiple_of(core * half, half)
    there = pl.multiple_of((1 - core) * half, half)
    near = near / norm + res[:, pl.ds(here, half)]
    far = far / norm + res[:, pl.ds(there, half)]
    total = jnp.sum(jnp.abs(near), axis=1, keepdims=True) + jnp.sum(jnp.abs(far), axis=1, keepdims=True)
    scale = (total / width + 1e-06).astype(BF16).astype(F32)
    for value, at in ((near, here), (far, there)):
        soft = jnp.tanh(value / scale).astype(BF16).astype(F32)
        decoded = scale * soft
        res_out[:, pl.ds(at, half)] = value - decoded
        dec[:, pl.ds(at, half)] = decoded.astype(BF16)


def vmem(n):
    return [pl.BlockSpec(memory_space=pltpu.VMEM)] * n


def smem():
    return pl.BlockSpec(memory_space=pltpu.SMEM)


def per_device(tokens, grad_out, gate_weight, down_weight, residual_in):
    shards, groups = lax.axis_size("fsdp"), lax.axis_size("rep")
    slab, width = gate_weight.shape
    half, chips = width // 2, shards // 2
    me, rep = lax.axis_index("fsdp"), lax.axis_index("rep")
    core, chip = me % 2, me // 2

    def partner(x):
        return lax.ppermute(x, "fsdp", [(i, i ^ 1) for i in range(shards)])

    def shift(x, k):
        return lax.ppermute(x, "fsdp", [(i, (i + 2 * k) % shards) for i in range(shards)])

    def swap(x, bit):
        return lax.ppermute(x, "rep", [(i, i ^ bit) for i in range(groups)])

    def columns(side):
        return jnp.stack([lax.dynamic_slice_in_dim(w, side * half, half, 1) for w in (gate_weight, down_weight)])

    own = columns(core)
    got = partner(columns(1 - core))
    part = 2 * slab // groups
    piece = lax.dynamic_slice_in_dim(jnp.concatenate([own, got], axis=1), rep * part, part, 1)
    pieces = {k: shift(piece, k) for k in range(1, chips)}
    t1, g1 = partner(tokens), partner(grad_out)

    def start_of(source, flat):
        side, row = flat // slab, flat % slab
        shard = 2 * source + jnp.where(side == 0, core, 1 - core)
        return shard * slab + row

    weights, places, starts = [], [], []
    for w in (0, 1):
        for side, array in ((0, own), (1, got)):
            weights.append(array[w])
            places.append(w)
            starts.append(start_of(chip, jnp.int32(side * slab)))
    for k in pieces:
        source = (chip - k) % chips
        for offset, pair in gather_rep(pieces[k], groups, swap).items():
            for w in (0, 1):
                weights.append(pair[w])
                places.append(w)
                starts.append(start_of(source, (rep ^ offset) * part))
    up = pl.pallas_call(
        lambda *refs: hidden_kernel(places, part, *refs),
        out_shape=jax.ShapeDtypeStruct((2 * tokens.shape[0], half), BF16),
        in_specs=[smem()] + vmem(4 + len(weights)),
        out_specs=pl.BlockSpec(memory_space=pltpu.VMEM),
        name="hidden",
    )(jnp.stack(starts).astype(jnp.int32), tokens, t1, grad_out, g1, *weights)

    def slab_of(target):
        at = (2 * target + core) * slab
        return jnp.stack([lax.dynamic_slice_in_dim(t, at, slab, 1) for t in (tokens, t1)])

    toks = [slab_of(chip)] + [shift(slab_of((chip + k) % chips), k) for k in range(1, chips)]
    mine = [up] + [shift(up, k) for k in range(1, chips)]
    theirs = [partner(u) for u in mine]
    norm = math.sqrt(tokens.shape[0] * shards)
    res_out, dec = pl.pallas_call(
        lambda *refs: update_kernel(norm, chips, *refs),
        out_shape=(jax.ShapeDtypeStruct((slab, width), F32), jax.ShapeDtypeStruct((slab, width), BF16)),
        in_specs=[smem()] + vmem(1 + 3 * chips),
        out_specs=tuple(vmem(2)),
        name="update",
    )(jnp.reshape(core, (1,)).astype(jnp.int32), residual_in[0], *toks, *mine, *theirs)
    bits = [1 << i for i in range((groups - 1).bit_length())]
    parts = [dec[: slab // 2], dec[slab // 2:]]
    for step in range(len(bits)):
        sent = [swap(parts[0], bits[step]), swap(parts[1], bits[::-1][step])]
        last = step + 1 == len(bits)
        parts = [p.astype(F32) + s.astype(F32) for p, s in zip(parts, sent)]
        if not last:
            parts = [p.astype(BF16) for p in parts]
    update = jnp.concatenate(parts, axis=0) / groups
    return (res_out[None], update)


def solution(mesh):
    in_specs = (
        P(("rep", "fsdp"), None),
        P(("rep", "fsdp"), None),
        P("fsdp", None),
        P("fsdp", None),
        P("rep", "fsdp", None),
    )
    out_specs = (P("rep", "fsdp", None), P("fsdp", None))
    return jax.shard_map(
        per_device, mesh=mesh, in_specs=in_specs, out_specs=out_specs, check_vma=False
    )
```
